32 devices in a mesh: dp: 1 (over z), row: 4 (over y), col: 8 (over x, core).
Axes of the slice: x: 4, y: 4, z: 1, core: 2. Of those that a mesh axis runs over, the one named last changes fastest.
The devices are a block of a 4x4x8 slice.
Arguments:
- pair_rep: bfloat16 [768, 768, 128], P(('dp', 'row'), 'col')
- res_mask: int32 [768], P('dp')
- ln_gamma: float32 [128], replicated
- ln_beta: float32 [128], replicated
- w_q: bfloat16 [128, 128], replicated
- w_k: bfloat16 [128, 128], replicated
- w_v: bfloat16 [128, 128], replicated
- w_b: bfloat16 [128, 4], replicated
- w_g: bfloat16 [128, 128], replicated
- w_o: bfloat16 [128, 128], replicated
Outputs:
- output: bfloat16 [768, 768, 128], P(('dp', 'row'), 'col')
All inputs are finite; a program needn't handle non-finite values.
Results may differ from the reference program's by a relative error of at most 0.00711597.
Values are sent between devices in bfloat16 or wider.
A program may use at most 768 MiB of HBM per device.

```python
import jax
import jax.numpy as jnp
from jax import lax

N = 768
C_Z = 128
HEADS = 4
HEAD = 32
LN_EPS = 1e-5


def layer_norm(pair_rep, ln_gamma, ln_beta):
    pair_f32 = pair_rep.astype(jnp.float32)
    mean_c = jnp.mean(pair_f32, axis=-1, keepdims=True)
    centered = pair_f32 - mean_c
    var_c = jnp.mean(jnp.square(centered), axis=-1, keepdims=True)
    return (centered * lax.rsqrt(var_c + LN_EPS) * ln_gamma + ln_beta).astype(jnp.bfloat16)


def setup_inputs(seed: int = 0, part: int = 0) -> dict:
    part_key = jax.random.fold_in(jax.random.key(seed), part)
    pair_key, len_key = jax.random.split(part_key)
    weight_keys = jax.random.split(jax.random.key(seed + 1), 8)
    proj_dim = HEADS * HEAD
    in_scale = C_Z ** -0.5
    pair_rep = jax.random.normal(pair_key, (N, N, C_Z), jnp.float32).astype(jnp.bfloat16)
    seq_len = jax.random.randint(len_key, (), N // 4, N - N // 8 + 1)
    res_mask = (jnp.arange(N) < seq_len).astype(jnp.int32)
    ln_gamma = 1.0 + 0.5 * jax.random.normal(weight_keys[0], (C_Z,), jnp.float32)
    ln_beta = 0.5 * jax.random.normal(weight_keys[1], (C_Z,), jnp.float32)
    w_q = (jax.random.normal(weight_keys[2], (C_Z, proj_dim), jnp.float32) * in_scale).astype(jnp.bfloat16)
    w_k = (jax.random.normal(weight_keys[3], (C_Z, proj_dim), jnp.float32) * in_scale).astype(jnp.bfloat16)
    w_v = (jax.random.normal(weight_keys[4], (C_Z, proj_dim), jnp.float32) * in_scale).astype(jnp.bfloat16)
    w_b = (jax.random.normal(weight_keys[5], (C_Z, HEADS), jnp.float32) * in_scale).astype(jnp.bfloat16)
    w_g = (jax.random.normal(weight_keys[6], (C_Z, proj_dim), jnp.float32) * in_scale).astype(jnp.bfloat16)
    w_o = (jax.random.normal(weight_keys[7], (proj_dim, C_Z), jnp.float32) * (4.0 * proj_dim ** -0.5)).astype(jnp.bfloat16)
    return {'pair_rep': pair_rep, 'res_mask': res_mask, 'ln_gamma': ln_gamma, 'ln_beta': ln_beta, 'w_q': w_q, 'w_k': w_k, 'w_v': w_v, 'w_b': w_b, 'w_g': w_g, 'w_o': w_o}


def reference(pair_rep, res_mask, ln_gamma, ln_beta, w_q, w_k, w_v, w_b, w_g, w_o):
    proj_dim = HEADS * HEAD
    normed = layer_norm(pair_rep, ln_gamma, ln_beta)
    pair_bias = jnp.dot(normed.reshape(N * N, C_Z), w_b, preferred_element_type=jnp.float32).astype(jnp.bfloat16)
    key_bias = jnp.where(res_mask > 0, 0.0, -1e9).astype(jnp.float32)
    full_bias = pair_bias.reshape(N, N, HEADS).astype(jnp.float32) + key_bias[None, :, None]

    def one_row(row_args):
        pair_row, normed_row = row_args
        queries = (jnp.dot(normed_row, w_q, preferred_element_type=jnp.float32) * HEAD ** -0.5).astype(jnp.bfloat16)
        key_row = jnp.dot(normed_row, w_k, preferred_element_type=jnp.float32).astype(jnp.bfloat16)
        val_row = jnp.dot(normed_row, w_v, preferred_element_type=jnp.float32).astype(jnp.bfloat16)
        gate_vals = jax.nn.sigmoid(jnp.dot(normed_row, w_g, preferred_element_type=jnp.float32))
        logits = jnp.einsum('jhd,khd->jkh', queries.reshape(N, HEADS, HEAD).astype(jnp.float32), key_row.reshape(N, HEADS, HEAD).astype(jnp.float32)) + full_bias
        weights = jax.nn.softmax(logits, axis=1)
        attended = jnp.einsum('jkh,khd->jhd', weights, val_row.reshape(N, HEADS, HEAD).astype(jnp.float32))
        gated_out = (gate_vals * attended.reshape(N, proj_dim)).astype(jnp.bfloat16)
        update = jnp.dot(gated_out, w_o, preferred_element_type=jnp.float32)
        return (pair_row.astype(jnp.float32) + update).astype(jnp.bfloat16)

    return lax.map(one_row, (pair_rep, normed))
```

```python
import functools

import jax
import jax.numpy as jnp
from jax import lax
from jax.experimental import pallas as pl
from jax.experimental.pallas import tpu as pltpu
from jax.sharding import PartitionSpec as P

LN_EPS = 1e-5
MASKED = -1e9
MESH = pl.DeviceIdType.MESH
GROUP = 32
QTILE = 256
KEYBLK = 128
CHUNKS = 4


def exchange_kernel(n_col, n_row, z_hbm, gamma_ref, beta_ref, stat_ref, wexp_ref,
                    rows_ref, ball_ref, zv, av, bt, load_sem, asend, arecv, bsend, brecv, own_sem):
    me = lax.axis_index('col')
    row = lax.axis_index('row')
    parts, rows, width, chan = zv.shape
    n_chip = n_col // 2
    partner = me + 1 - 2 * lax.rem(me, 2)

    loads = []
    order = [2, n_col - 2]
    order += [k for k in range(1, n_col) if k not in order] + [0]
    dests = [lax.rem(me + k, n_col) for k in order]
    for slot, dest in enumerate(dests):
        load = pltpu.make_async_copy(z_hbm.at[dest], zv.at[slot], load_sem.at[slot])
        load.start()
        loads.append(load)

    barrier = pltpu.get_barrier_semaphore()
    for k in range(1, n_col):
        pl.semaphore_signal(barrier, inc=1, device_id={'col': lax.rem(me + k, n_col)}, device_id_type=MESH)
    for k in range(1, n_row):
        pl.semaphore_signal(barrier, inc=1, device_id={'row': lax.rem(row + k, n_row)}, device_id_type=MESH)
    pl.semaphore_wait(barrier, n_col + n_row - 2)

    gamma = gamma_ref[...]
    beta = beta_ref[...]
    step_rows = 4

    def norm_part(slot, dest):
        def body(step, carry):
            base = step * step_rows
            z_bf = zv[slot, pl.ds(base, step_rows)].reshape(step_rows * width, chan)
            mean = jnp.dot(z_bf, stat_ref[:chan], preferred_element_type=jnp.float32)
            cent = z_bf.astype(jnp.float32) - mean
            sq = cent * cent
            hi = sq.astype(jnp.bfloat16)
            lo = (sq - hi.astype(jnp.float32)).astype(jnp.bfloat16)
            var = jnp.dot(jnp.concatenate([hi, lo], axis=-1), stat_ref[...], preferred_element_type=jnp.float32)
            normed = cent * lax.rsqrt(var + LN_EPS) * gamma + beta
            av[dest, pl.ds(base, step_rows)] = normed.astype(jnp.bfloat16).reshape(step_rows, width, chan)
            return carry
        lax.fori_loop(0, rows // step_rows, body, 0)

    def row_copy(slot):
        dest = dests[slot]
        return pltpu.make_async_remote_copy(
            av.at[dest], rows_ref.at[me], asend.at[slot], arecv.at[slot],
            device_id={'col': dest}, device_id_type=MESH)

    early = 2
    for slot, dest in enumerate(dests):
        loads[slot].wait()
        norm_part(slot, dest)
        if slot < early:
            row_copy(slot).start()
    own = pltpu.make_async_copy(av.at[me], rows_ref.at[me], own_sem.at[0])
    own.start()

    tile_rows = parts * rows
    heads = bt.shape[0]
    for grp in range(tile_rows // GROUP):
        flat = [av[(grp * GROUP + jj) // rows, (grp * GROUP + jj) % rows] for jj in range(GROUP)]
        res = jnp.dot(jnp.concatenate(flat, axis=-1), wexp_ref[...], preferred_element_type=jnp.float32)
        for h in range(heads):
            bt[h, :, grp * GROUP:(grp + 1) * GROUP] = res[:, h * GROUP:(h + 1) * GROUP].astype(jnp.bfloat16)

    own_b = pltpu.make_async_copy(bt, ball_ref.at[row, me], own_sem.at[1])
    own_b.start()

    def b_copy(src, src_row, src_col, kind, device):
        return pltpu.make_async_remote_copy(
            src, ball_ref.at[src_row, src_col], bsend.at[kind], brecv.at[kind],
            device_id=device, device_id_type=MESH)

    x_slot = lambda m: m - 1
    y_slot = lambda s, m: (n_chip - 1) + (s - 1) * n_chip + m
    p_slot = lambda s, m: (n_chip - 1) + (n_row - 1) * n_chip + s * n_chip + m
    sent = []
    for m in range(1, n_chip):
        cp = b_copy(bt, row, me, x_slot(m), {'col': lax.rem(me + 2 * m, n_col)})
        cp.start()
        sent.append(cp)
    for s in range(1, n_row):
        cp = b_copy(bt, row, me, y_slot(s, 0), {'row': lax.rem(row + s, n_row)})
        cp.start()
        sent.append(cp)
    cp = b_copy(bt, row, me, p_slot(0, 0), {'col': partner})
    cp.start()
    sent.append(cp)
    for slot in range(early, n_col - 1):
        row_copy(slot).start()

    def block_at(s, m):
        src_row = lax.rem(row + n_row - s, n_row)
        src_col = lax.rem(me + n_col - 2 * m, n_col)
        return src_row, src_col

    for m in range(1, n_chip):
        src_row, src_col = block_at(0, m)
        block = ball_ref.at[src_row, src_col]
        pltpu.make_async_remote_copy(block, block, bsend.at[x_slot(m)], brecv.at[x_slot(m)],
                                     device_id={'col': partner}, device_id_type=MESH).wait_recv()
        for s in range(1, n_row):
            cp = b_copy(block, src_row, src_col, y_slot(s, m), {'row': lax.rem(row + s, n_row)})
            cp.start()
            sent.append(cp)
        cp = b_copy(block, src_row, src_col, p_slot(0, m), {'col': partner})
        cp.start()
        sent.append(cp)
    for m in range(n_chip):
        for s in range(1, n_row):
            src_row, src_col = block_at(s, m)
            block = ball_ref.at[src_row, src_col]
            pltpu.make_async_remote_copy(block, block, bsend.at[y_slot(s, m)], brecv.at[y_slot(s, m)],
                                         device_id={'col': partner}, device_id_type=MESH).wait_recv()
            cp = b_copy(block, src_row, src_col, p_slot(s, m), {'col': partner})
            cp.start()
            sent.append(cp)
    for m in range(n_chip):
        for s in range(n_row):
            src_row = lax.rem(row + n_row - s, n_row)
            src_col = lax.rem(partner + n_col - 2 * m, n_col)
            block = ball_ref.at[src_row, src_col]
            pltpu.make_async_remote_copy(block, block, bsend.at[p_slot(s, m)], brecv.at[p_slot(s, m)],
                                         device_id={'col': partner}, device_id_type=MESH).wait_recv()
    for cp in sent:
        cp.wait_send()
    own_b.wait()
    own.wait()
    for slot in range(n_col - 1):
        row_copy(slot).wait()


def exchange(n_col, n_row, pair_tile, gamma, beta, stat, wexp, heads):
    row_len, width, chan = pair_tile.shape
    rows = row_len // n_col
    n_bsem = (n_col // 2 - 1) + (n_row - 1) * (n_col // 2) + n_row * (n_col // 2)
    hbm = pl.BlockSpec(memory_space=pl.ANY)
    vmem = pl.BlockSpec(memory_space=pltpu.VMEM)
    return pl.pallas_call(
        functools.partial(exchange_kernel, n_col, n_row),
        name='exchange_rows',
        out_shape=(jax.ShapeDtypeStruct((n_col, rows, width, chan), jnp.bfloat16),
                   jax.ShapeDtypeStruct((n_row, n_col, heads, width, row_len), jnp.bfloat16)),
        in_specs=[hbm, vmem, vmem, vmem, vmem],
        out_specs=(hbm, hbm),
        scratch_shapes=[
            pltpu.VMEM((n_col, rows, width, chan), jnp.bfloat16),
            pltpu.VMEM((n_col, rows, width, chan), jnp.bfloat16),
            pltpu.VMEM((heads, width, row_len), jnp.bfloat16),
            pltpu.SemaphoreType.DMA((n_col,)),
            pltpu.SemaphoreType.DMA((n_col,)),
            pltpu.SemaphoreType.DMA((n_col,)),
            pltpu.SemaphoreType.DMA((n_bsem,)),
            pltpu.SemaphoreType.DMA((n_bsem,)),
            pltpu.SemaphoreType.DMA((2,)),
        ],
        compiler_params=pltpu.CompilerParams(collective_id=1, has_side_effects=True, vmem_limit_bytes=48 << 20),
    )(pair_tile.reshape(n_col, rows, width, chan), gamma, beta, stat, wexp)


def attend_kernel(scale, nblk_ref, a_ref, ball_ref, mask_ref, wk_ref, wqvg_ref, out_ref,
                  bias, kbuf, qz, vt, gt, og):
    n_row, n_col, heads, width, row_len = ball_ref.shape
    keys = n_col * width
    chan = a_ref.shape[-1]
    head_dim = chan // heads

    @pl.when(pl.program_id(0) == 0)
    def _():
        qz[...] = jnp.zeros_like(qz)

        def fill(c, carry):
            krange = pl.ds(pl.multiple_of(c * width, width), width)
            mask = mask_ref[krange, :1]
            for h in range(heads):
                for r in range(n_row):
                    bias[h, krange, r * row_len:(r + 1) * row_len] = ball_ref[r, c, h].astype(jnp.float32) + mask
            return carry
        lax.fori_loop(0, n_col, fill, 0)

    a = a_ref[:, 0].reshape(keys, chan)
    kbuf[...] = jnp.dot(a, wk_ref[...], preferred_element_type=jnp.float32).astype(jnp.bfloat16)
    qvg = lax.dot_general(wqvg_ref[...], a, (((1,), (1,)), ((), ())), preferred_element_type=jnp.float32)
    q_t = (qvg[:chan] * scale).astype(jnp.bfloat16)
    v_t = qvg[chan:2 * chan].astype(jnp.bfloat16)
    gt[...] = jax.nn.sigmoid(qvg[2 * chan:]).reshape(heads, head_dim, keys)
    for h in range(heads):
        qz[h, h * head_dim:(h + 1) * head_dim, :] = q_t[h * head_dim:(h + 1) * head_dim]
        vt[h] = v_t[h * head_dim:(h + 1) * head_dim]

    def attend(nk):
        def head(h, carry):
            for qt in range(keys // QTILE):
                cols = slice(qt * QTILE, (qt + 1) * QTILE)
                s = jnp.dot(kbuf[:nk], qz[h, :, cols], preferred_element_type=jnp.float32) + bias[h, :nk, cols]
                m = jnp.max(s, axis=0, keepdims=True)
                p = jnp.exp(s - m)
                l = jnp.sum(p, axis=0, keepdims=True)
                o = jnp.dot(vt[h, :, :nk], p.astype(jnp.bfloat16), preferred_element_type=jnp.float32)
                og[h, :, cols] = gt[h, :, cols] * (o / l)
            return carry
        lax.fori_loop(0, heads, head, 0)

    for nblk in range(1, keys // KEYBLK + 1):
        @pl.when(nblk_ref[0] == nblk)
        def _():
            attend(nblk * KEYBLK)

    gated = og[...].reshape(chan, keys).T
    out_ref[:, 0] = gated.astype(jnp.bfloat16).reshape(n_col, width, chan)


def attend(first, count, nblk, a_rows, ball, mask, w_k, w_qvg, scale):
    n_col, rows, width, chan = a_rows.shape
    n_row, _, heads, _, row_len = ball.shape
    keys = n_col * width
    head_dim = chan // heads
    const = lambda shape: pl.BlockSpec(shape, lambda g, s: (0,) * len(shape), pipeline_mode=pl.Buffered(1))
    grid_spec = pltpu.PrefetchScalarGridSpec(
        num_scalar_prefetch=1,
        grid=(count,),
        in_specs=[
            pl.BlockSpec((n_col, 1, width, chan), lambda g, s: (0, first + g, 0, 0)),
            const(ball.shape), const(mask.shape), const(w_k.shape), const(w_qvg.shape),
        ],
        out_specs=pl.BlockSpec((n_col, 1, width, chan), lambda g, s: (0, g, 0, 0)),
        scratch_shapes=[
            pltpu.VMEM((heads, keys, keys), jnp.float32),
            pltpu.VMEM((keys, chan), jnp.bfloat16),
            pltpu.VMEM((heads, chan, keys), jnp.bfloat16),
            pltpu.VMEM((heads, head_dim, keys), jnp.bfloat16),
            pltpu.VMEM((heads, head_dim, keys), jnp.float32),
            pltpu.VMEM((heads, head_dim, keys), jnp.float32),
        ])
    flops = count * (4 * keys * keys * chan * 2 + 8 * keys * chan * chan)
    return pl.pallas_call(
        functools.partial(attend_kernel, scale),
        name='attend_rows',
        grid_spec=grid_spec,
        out_shape=jax.ShapeDtypeStruct((n_col, count, width, chan), jnp.bfloat16),
        cost_estimate=pl.CostEstimate(flops=flops * 20, bytes_accessed=ball.size * 2 + count * keys * chan * 4,
                                      transcendentals=count * heads * keys * keys),
        compiler_params=pltpu.CompilerParams(dimension_semantics=('arbitrary',), vmem_limit_bytes=56 << 20),
    )(nblk, a_rows, ball, mask, w_k, w_qvg)


def finish_kernel(z_ref, g_ref, wo_ref, *rest):
    out_ref = rest[-1]
    _, count, width, chan = z_ref.shape
    upd = jnp.dot(g_ref[0].reshape(count * width, chan), wo_ref[...], preferred_element_type=jnp.float32)
    z = z_ref[0].reshape(count * width, chan).astype(jnp.float32)
    out_ref[0] = (z + upd).astype(jnp.bfloat16).reshape(count, width, chan)


def finish(idx, count, z_parts, gated, w_o, prev):
    n_col, rows, width, chan = z_parts.shape
    blk = pl.BlockSpec((1, count, width, chan), lambda d: (d, idx, 0, 0))
    in_specs = [blk, pl.BlockSpec((1, count, width, chan), lambda d: (d, 0, 0, 0)),
                pl.BlockSpec(w_o.shape, lambda d: (0, 0))]
    args = [z_parts, gated, w_o]
    alias = {}
    if prev is not None:
        in_specs.append(pl.BlockSpec(memory_space=pl.ANY))
        args.append(prev)
        alias = {3: 0}
    return pl.pallas_call(
        finish_kernel, name='finish_rows', grid=(n_col,), in_specs=in_specs, out_specs=blk,
        out_shape=jax.ShapeDtypeStruct(z_parts.shape, z_parts.dtype),
        input_output_aliases=alias,
        cost_estimate=pl.CostEstimate(flops=n_col * count * width * chan * chan * 2 * 4, transcendentals=0,
                                      bytes_accessed=n_col * count * width * chan * 6),
        compiler_params=pltpu.CompilerParams(dimension_semantics=('arbitrary',)),
    )(*args)


def needed_blocks(res_mask, ln_gamma, ln_beta, w_q, w_k, w_b, n_blocks):
    chan, heads = w_b.shape
    amax = (chan ** 0.5 * jnp.abs(ln_gamma) + jnp.abs(ln_beta)) * 1.01
    w_all = jnp.concatenate([w_q, w_k, w_b], axis=1).astype(jnp.float32)
    top = jnp.sum(amax[:, None] * jnp.abs(w_all), axis=0) * 1.01
    head_dim = w_q.shape[1] // heads
    qk = jnp.sum(top[:w_q.shape[1]] * top[w_q.shape[1]:2 * w_q.shape[1]]) * head_dim ** -0.5
    bound = qk + jnp.sum(top[2 * w_q.shape[1]:])
    valid = jnp.sum((res_mask > 0).astype(jnp.int32))
    nblk = jnp.where(bound < -0.4 * MASKED, (valid + KEYBLK - 1) // KEYBLK, n_blocks)
    return jnp.clip(nblk, 1, n_blocks).astype(jnp.int32).reshape(1)


def solution(mesh):
    n_col, n_row = mesh.shape['col'], mesh.shape['row']
    tile_spec = P(('dp', 'row'), 'col', None)

    def per_device(pair_tile, res_mask, ln_gamma, ln_beta, w_q, w_k, w_v, w_b, w_g, w_o):
        row_len, width, chan = pair_tile.shape
        heads = w_b.shape[1]
        keys = n_col * width
        scale = (w_q.shape[1] // heads) ** -0.5
        rows = row_len // n_col
        stat = jnp.full((2 * chan, chan), 1.0 / chan, jnp.bfloat16)
        lane = jnp.arange(heads * GROUP)
        sel = (lane[None, :] % GROUP == jnp.arange(GROUP)[:, None])
        w_rep = jnp.repeat(w_b, GROUP, axis=1)
        wexp = jnp.where(sel[:, None, :], w_rep[None], 0).astype(jnp.bfloat16).reshape(GROUP * chan, heads * GROUP)
        a_rows, ball = exchange(n_col, n_row, pair_tile, ln_gamma.reshape(1, chan), ln_beta.reshape(1, chan),
                                stat, wexp, heads)
        mask = jnp.broadcast_to(jnp.where(res_mask > 0, 0.0, MASKED).astype(jnp.float32)[:, None], (keys, 128))
        w_qvg = jnp.concatenate([w_q.T, w_v.T, w_g.T], axis=0)
        nblk = needed_blocks(res_mask, ln_gamma, ln_beta, w_q, w_k, w_b, keys // KEYBLK)
        z_parts = pair_tile.reshape(n_col, rows, width, chan)
        count = rows // CHUNKS
        home = []
        for t in range(CHUNKS):
            gated = attend(t * count, count, nblk, a_rows, ball, mask, w_k, w_qvg, scale)
            home.append(lax.all_to_all(gated, 'col', 0, 0, tiled=True))
        out = None
        for t in range(CHUNKS):
            out = finish(t, count, z_parts, home[t], w_o, out)
        return out.reshape(row_len, width, chan)

    return jax.shard_map(per_device, mesh=mesh, in_specs=(tile_spec, P('dp'), P(), P(), P(), P(), P(), P(), P(), P()), out_specs=tile_spec, check_vma=False)
```

```python
import functools

import jax
import jax.numpy as jnp
from jax import lax
from jax.experimental import pallas as pl
from jax.experimental.pallas import tpu as pltpu
from jax.sharding import PartitionSpec as P


LN_EPS = 1e-5
MASKED = -1e9
SAFE = 1e-15
MESH = pl.DeviceIdType.MESH
GROUP = 32
QTILE = 256
KEYBLK = 128
EARLY = 2
VMEM_ALL = 67043328
PAIR = 2
UNROLL = 4
SHARES = (2, 1)


def exchange_kernel(n_col, n_row, z_hbm, gamma_ref, beta_ref, wrep_ref,
                    rows_ref, ball_ref, zv, av, bt, wexp_ref, load_sem, asend, arecv, bsend, brecv, own_sem):
    me = lax.axis_index('col')
    row = lax.axis_index('row')
    parts, rows, width, chan = zv.shape
    n_chip = n_col // 2
    partner = me + 1 - 2 * lax.rem(me, 2)

    loads = []
    order = [2, n_col - 2, n_col // 2]
    order += [k for k in range(1, n_col) if k not in order] + [0]
    dests = [lax.rem(me + k, n_col) for k in order]
    for slot, dest in enumerate(dests):
        load = pltpu.make_async_copy(z_hbm.at[dest], zv.at[slot], load_sem.at[slot])
        load.start()
        loads.append(load)

    barrier = pltpu.get_barrier_semaphore()
    for k in range(1, n_col):
        pl.semaphore_signal(barrier, inc=1, device_id={'col': lax.rem(me + k, n_col)}, device_id_type=MESH)
    for k in range(1, n_row):
        pl.semaphore_signal(barrier, inc=1, device_id={'row': lax.rem(row + k, n_row)}, device_id_type=MESH)
    pl.semaphore_wait(barrier, n_col + n_row - 2)

    stat = jnp.full((2 * chan, chan), 1.0 / chan, jnp.bfloat16)
    gamma = gamma_ref[...]
    beta = beta_ref[...]
    step_rows = rows // 2

    def norm_part(slot, dest):
        def body(step, carry):
            base = step * step_rows
            z_bf = zv[slot, pl.ds(base, step_rows)].reshape(step_rows * width, chan)
            mean = jnp.dot(z_bf, stat[:chan], preferred_element_type=jnp.float32)
            cent = z_bf.astype(jnp.float32) - mean
            sq = cent * cent
            hi = sq.astype(jnp.bfloat16)
            lo = (sq - hi.astype(jnp.float32)).astype(jnp.bfloat16)
            var = jnp.dot(jnp.concatenate([hi, lo], axis=-1), stat, preferred_element_type=jnp.float32)
            normed = cent * lax.rsqrt(var + LN_EPS) * gamma + beta
            av[dest, pl.ds(base, step_rows)] = normed.astype(jnp.bfloat16).reshape(step_rows, width, chan)
            return carry

        lax.fori_loop(0, rows // step_rows, body, 0)

    def row_copy(slot):
        dest = dests[slot]
        return pltpu.make_async_remote_copy(
            av.at[dest], rows_ref.at[me], asend.at[slot], arecv.at[slot],
            device_id={'col': dest}, device_id_type=MESH)

    early = EARLY
    for slot, dest in enumerate(dests):
        loads[slot].wait()
        norm_part(slot, dest)
        if slot < early:
            row_copy(slot).start()
    own = pltpu.make_async_copy(av.at[me], rows_ref.at[me], own_sem.at[0])
    own.start()

    lane = lax.broadcasted_iota(jnp.int32, wrep_ref.shape, 1)
    for jj in range(GROUP):
        wexp_ref[jj * chan:(jj + 1) * chan] = jnp.where(lax.rem(lane, GROUP) == jj, wrep_ref[...], 0.0).astype(jnp.bfloat16)
    tile_rows = parts * rows
    heads = bt.shape[0]
    for grp in range(tile_rows // GROUP):
        flat = [av[(grp * GROUP + jj) // rows, (grp * GROUP + jj) % rows] for jj in range(GROUP)]
        res = jnp.dot(jnp.concatenate(flat, axis=-1), wexp_ref[...], preferred_element_type=jnp.float32)
        for h in range(heads):
            bt[h, :, grp * GROUP:(grp + 1) * GROUP] = res[:, h * GROUP:(h + 1) * GROUP].astype(jnp.bfloat16)

    own_b = pltpu.make_async_copy(bt, ball_ref.at[row, me], own_sem.at[1])
    own_b.start()

    def b_copy(src, src_row, src_col, kind, device):
        return pltpu.make_async_remote_copy(
            src, ball_ref.at[src_row, src_col], bsend.at[kind], brecv.at[kind],
            device_id=device, device_id_type=MESH)

    x_slot = lambda m: m - 1
    y_slot = lambda s, m: (n_chip - 1) + (s - 1) * n_chip + m
    p_slot = lambda s, m: (n_chip - 1) + (n_row - 1) * n_chip + s * n_chip + m
    sent = []
    for m in range(1, n_chip):
        cp = b_copy(bt, row, me, x_slot(m), {'col': lax.rem(me + 2 * m, n_col)})
        cp.start()
        sent.append(cp)
    for s in range(1, n_row):
        cp = b_copy(bt, row, me, y_slot(s, 0), {'row': lax.rem(row + s, n_row)})
        cp.start()
        sent.append(cp)
    cp = b_copy(bt, row, me, p_slot(0, 0), {'col': partner})
    cp.start()
    sent.append(cp)
    for slot in range(early, n_col - 1):
        row_copy(slot).start()

    def block_at(s, m):
        src_row = lax.rem(row + n_row - s, n_row)
        src_col = lax.rem(me + n_col - 2 * m, n_col)
        return src_row, src_col

    for m in range(1, n_chip):
        src_row, src_col = block_at(0, m)
        block = ball_ref.at[src_row, src_col]
        pltpu.make_async_remote_copy(block, block, bsend.at[x_slot(m)], brecv.at[x_slot(m)],
                                     device_id={'col': partner}, device_id_type=MESH).wait_recv()
        for s in range(1, n_row):
            cp = b_copy(block, src_row, src_col, y_slot(s, m), {'row': lax.rem(row + s, n_row)})
            cp.start()
            sent.append(cp)
        cp = b_copy(block, src_row, src_col, p_slot(0, m), {'col': partner})
        cp.start()
        sent.append(cp)
    for m in range(n_chip):
        for s in range(1, n_row):
            src_row, src_col = block_at(s, m)
            block = ball_ref.at[src_row, src_col]
            pltpu.make_async_remote_copy(block, block, bsend.at[y_slot(s, m)], brecv.at[y_slot(s, m)],
                                         device_id={'col': partner}, device_id_type=MESH).wait_recv()
            cp = b_copy(block, src_row, src_col, p_slot(s, m), {'col': partner})
            cp.start()
            sent.append(cp)
    for m in range(n_chip):
        for s in range(n_row):
            src_row = lax.rem(row + n_row - s, n_row)
            src_col = lax.rem(partner + n_col - 2 * m, n_col)
            block = ball_ref.at[src_row, src_col]
            pltpu.make_async_remote_copy(block, block, bsend.at[p_slot(s, m)], brecv.at[p_slot(s, m)],
                                         device_id={'col': partner}, device_id_type=MESH).wait_recv()
    for cp in sent:
        cp.wait_send()
    own_b.wait()
    own.wait()
    for slot in range(n_col - 1):
        row_copy(slot).wait()


def exchange(n_col, n_row, pair_tile, gamma, beta, w_rep, heads):
    row_len, width, chan = pair_tile.shape
    rows = row_len // n_col
    n_bsem = (n_col // 2 - 1) + (n_row - 1) * (n_col // 2) + n_row * (n_col // 2)
    hbm = pl.BlockSpec(memory_space=pl.ANY)
    vmem = pl.BlockSpec(memory_space=pltpu.VMEM)
    return pl.pallas_call(
        functools.partial(exchange_kernel, n_col, n_row),
        name='exchange_rows',
        out_shape=(jax.ShapeDtypeStruct((n_col, rows, width, chan), jnp.bfloat16),
                   jax.ShapeDtypeStruct((n_row, n_col, heads, width, row_len), jnp.bfloat16)),
        in_specs=[hbm, vmem, vmem, vmem],
        out_specs=(hbm, hbm),
        scratch_shapes=[
            pltpu.VMEM((n_col, rows, width, chan), jnp.bfloat16),
            pltpu.VMEM((n_col, rows, width, chan), jnp.bfloat16),
            pltpu.VMEM((heads, width, row_len), jnp.bfloat16),
            pltpu.VMEM((GROUP * chan, heads * GROUP), jnp.bfloat16),
            pltpu.SemaphoreType.DMA((n_col,)),
            pltpu.SemaphoreType.DMA((n_col,)),
            pltpu.SemaphoreType.DMA((n_col,)),
            pltpu.SemaphoreType.DMA((n_bsem,)),
            pltpu.SemaphoreType.DMA((n_bsem,)),
            pltpu.SemaphoreType.DMA((2,)),
        ],
        compiler_params=pltpu.CompilerParams(collective_id=1, has_side_effects=True, vmem_limit_bytes=VMEM_ALL),
    )(pair_tile.reshape(n_col, rows, width, chan), gamma, beta, w_rep)


def attend_kernel(scale, a_ref, ball_ref, mask_ref, wq_ref, wk_ref, wv_ref, wg_ref, out_ref,
                  wqvg_ref, bias, kbuf, qz, vt, gt, og, edge, mcol):
    n_row, n_col, heads, width, row_len = ball_ref.shape
    keys = n_col * width
    chan = a_ref.shape[-1]
    head_dim = chan // heads

    @pl.when(pl.program_id(0) == 0)
    def _():
        qz[...] = jnp.zeros_like(qz)
        for n, w_ref in enumerate((wq_ref, wv_ref, wg_ref)):
            wqvg_ref[n * chan:(n + 1) * chan] = w_ref[...].astype(jnp.float32).T.astype(jnp.bfloat16)
        added = jnp.where(mask_ref[...] > 0, 0.0, MASKED).astype(jnp.float32)
        mcol[...] = jnp.broadcast_to(added, (chan, keys)).T

        def fill(c, carry):
            krange = pl.ds(pl.multiple_of(c * width, width), width)
            mask = mcol[krange, :1]
            for h in range(heads):
                for r in range(n_row):
                    bias[h, krange, r * row_len:(r + 1) * row_len] = ball_ref[r, c, h].astype(jnp.float32) + mask
            return carry

        lax.fori_loop(0, n_col, fill, 0)

    pair = a_ref.shape[1]
    for r in range(pair):
        a = a_ref[:, r].reshape(keys, chan)
        kbuf[r] = jnp.dot(a, wk_ref[...], preferred_element_type=jnp.float32).astype(jnp.bfloat16)
        qvg = lax.dot_general(wqvg_ref[...], a, (((1,), (1,)), ((), ())), preferred_element_type=jnp.float32)
        q_t = (qvg[:chan] * scale).astype(jnp.bfloat16)
        v_t = qvg[chan:2 * chan].astype(jnp.bfloat16)
        gt[r] = jax.nn.sigmoid(qvg[2 * chan:]).reshape(heads, head_dim, keys)
        for h in range(heads):
            qz[r, h, h * head_dim:(h + 1) * head_dim, :] = q_t[h * head_dim:(h + 1) * head_dim]
            vt[r, h] = v_t[h * head_dim:(h + 1) * head_dim]

    def attend(nk):
        def heads_of(step, worst):
            low, high = worst
            r = step // (heads // UNROLL)
            for u in range(UNROLL):
                h = lax.rem(step, heads // UNROLL) * UNROLL + u
                for qt in range(keys // QTILE):
                    cols = slice(qt * QTILE, (qt + 1) * QTILE)
                    q_h = qz[r, h, :, cols]
                    total = None
                    parts = []
                    for kb in range(nk // KEYBLK):
                        kr = slice(kb * KEYBLK, (kb + 1) * KEYBLK)
                        s = jnp.dot(kbuf[r, kr], q_h, preferred_element_type=jnp.float32) + bias[h, kr, cols]
                        p = jnp.exp(s)
                        fold = jnp.sum(p.reshape(KEYBLK // 8, 8, QTILE), axis=0)
                        total = fold if total is None else total + fold
                        parts.append(p.astype(jnp.bfloat16))
                    l = jnp.sum(total, axis=0, keepdims=True)
                    o = jnp.dot(vt[r, h, :, :nk], jnp.concatenate(parts, axis=0), preferred_element_type=jnp.float32)
                    og[r, h, :, cols] = gt[r, h, :, cols] * (o / l)
                    low = jnp.minimum(low, l)
                    high = jnp.maximum(high, jnp.maximum(l, jnp.max(jnp.abs(o), axis=0, keepdims=True)))
            return low, high

        low, high = lax.fori_loop(0, pair * heads // UNROLL, heads_of, (jnp.full((1, QTILE), 1.0, jnp.float32),) * 2)
        edge[0:1] = low
        edge[1:2] = 1.0 / high

    def attend_exact(nk):
        def head(step, carry):
            r, h = step // heads, lax.rem(step, heads)
            for qt in range(keys // QTILE):
                cols = slice(qt * QTILE, (qt + 1) * QTILE)
                s = jnp.dot(kbuf[r, :nk], qz[r, h, :, cols], preferred_element_type=jnp.float32) + bias[h, :nk, cols]
                m = jnp.max(s, axis=0, keepdims=True)
                p = jnp.exp(s - m)
                l = jnp.sum(p, axis=0, keepdims=True)
                o = jnp.dot(vt[r, h, :, :nk], p.astype(jnp.bfloat16), preferred_element_type=jnp.float32)
                og[r, h, :, cols] = gt[r, h, :, cols] * (o / l)
            return carry

        lax.fori_loop(0, pair * heads, head, 0)

    attend(keys)

    @pl.when(jnp.logical_not(jnp.min(edge[...]) > SAFE))
    def _():
        attend_exact(keys)

    for r in range(pair):
        gated = og[r].reshape(chan, keys).T
        out_ref[:, r] = gated.astype(jnp.bfloat16).reshape(n_col, width, chan)


def attend(first, count, a_rows, ball, mask, weights, scale):
    n_col, _, width, chan = a_rows.shape
    _, _, heads, _, _ = ball.shape
    keys = n_col * width
    head_dim = chan // heads
    const = lambda shape: pl.BlockSpec(shape, lambda g: (0,) * len(shape), pipeline_mode=pl.Buffered(1))
    grid_spec = pltpu.PrefetchScalarGridSpec(
        num_scalar_prefetch=0,
        grid=(count // PAIR,),
        in_specs=[
            pl.BlockSpec((n_col, PAIR, width, chan), lambda g: (0, first // PAIR + g, 0, 0)),
            const(ball.shape), const(mask.shape), *[const(w.shape) for w in weights],
        ],
        out_specs=pl.BlockSpec((n_col, PAIR, width, chan), lambda g: (0, g, 0, 0)),
        scratch_shapes=[
            pltpu.VMEM((3 * chan, chan), jnp.bfloat16),
            pltpu.VMEM((heads, keys, keys), jnp.float32),
            pltpu.VMEM((PAIR, keys, chan), jnp.bfloat16),
            pltpu.VMEM((PAIR, heads, chan, keys), jnp.bfloat16),
            pltpu.VMEM((PAIR, heads, head_dim, keys), jnp.bfloat16),
            pltpu.VMEM((PAIR, heads, head_dim, keys), jnp.float32),
            pltpu.VMEM((PAIR, heads, head_dim, keys), jnp.float32),
            pltpu.VMEM((2, QTILE), jnp.float32),
            pltpu.VMEM((keys, chan), jnp.float32),
        ])
    flops = count * (4 * keys * keys * chan * 2 + 8 * keys * chan * chan)
    return pl.pallas_call(
        functools.partial(attend_kernel, scale),
        name='attend_rows',
        grid_spec=grid_spec,
        out_shape=jax.ShapeDtypeStruct((n_col, count, width, chan), jnp.bfloat16),
        cost_estimate=pl.CostEstimate(flops=flops * 20, bytes_accessed=ball.size * 2 + count * keys * chan * 4,
                                      transcendentals=count * heads * keys * keys),
        compiler_params=pltpu.CompilerParams(dimension_semantics=('arbitrary',), vmem_limit_bytes=VMEM_ALL),
    )(a_rows, ball, mask, *weights)


def finish_kernel(z_ref, g_ref, wo_ref, *rest):
    out_ref = rest[-1]
    parts, count, width, chan = z_ref.shape
    for d in range(parts):
        upd = jnp.dot(g_ref[d].reshape(count * width, chan), wo_ref[...], preferred_element_type=jnp.float32)
        z = z_ref[d].reshape(count * width, chan).astype(jnp.float32)
        out_ref[d] = (z + upd).astype(jnp.bfloat16).reshape(count, width, chan)


def finish(first, count, z_parts, gated, w_o, prev):
    n_col, _, width, chan = z_parts.shape
    parts = n_col // 2
    unit = 4
    blk = pl.BlockSpec((parts, unit, width, chan), lambda d, r: (d, first // unit + r, 0, 0))
    in_specs = [blk, pl.BlockSpec((parts, unit, width, chan), lambda d, r: (d, r, 0, 0)),
                pl.BlockSpec(w_o.shape, lambda d, r: (0, 0))]
    args = [z_parts, gated, w_o]
    alias = {}
    if prev is not None:
        in_specs.append(pl.BlockSpec(memory_space=pl.ANY))
        args.append(prev)
        alias = {3: 0}
    return pl.pallas_call(
        finish_kernel, name='finish_rows', grid=(n_col // parts, count // unit), in_specs=in_specs, out_specs=blk,
        out_shape=jax.ShapeDtypeStruct(z_parts.shape, z_parts.dtype),
        input_output_aliases=alias,
        cost_estimate=pl.CostEstimate(flops=n_col * count * width * chan * chan * 2 * 4, transcendentals=0,
                                      bytes_accessed=n_col * count * width * chan * 6),
        compiler_params=pltpu.CompilerParams(dimension_semantics=('arbitrary', 'arbitrary'), vmem_limit_bytes=VMEM_ALL),
    )(*args)


def solution(mesh):
    n_col, n_row = mesh.shape['col'], mesh.shape['row']
    tile_spec = P(('dp', 'row'), 'col', None)

    def per_device(pair_tile, res_mask, ln_gamma, ln_beta, w_q, w_k, w_v, w_b, w_g, w_o):
        row_len, width, chan = pair_tile.shape
        heads = w_b.shape[1]
        keys = n_col * width
        scale = (w_q.shape[1] // heads) ** -0.5
        rows = row_len // n_col
        w_rep = jnp.repeat(w_b.astype(jnp.float32), GROUP, axis=1)
        a_rows, ball = exchange(n_col, n_row, pair_tile, ln_gamma.reshape(1, chan), ln_beta.reshape(1, chan), w_rep, heads)
        mask = res_mask.reshape(1, keys)
        z_parts = pair_tile.reshape(n_col, rows, width, chan)
        home, first = [], 0
        for share in SHARES:
            count = rows * share // sum(SHARES)
            gated = attend(first, count, a_rows, ball, mask, (w_q, w_k, w_v, w_g), scale)
            home.append((first, count, lax.all_to_all(gated, 'col', 0, 0, tiled=True)))
            first += count
        out = None
        for first, count, gated in home:
            out = finish(first, count, z_parts, gated, w_o, out)
        return out.reshape(row_len, width, chan)

    return jax.shard_map(per_device, mesh=mesh, in_specs=(tile_spec, P('dp'), P(), P(), P(), P(), P(), P(), P(), P()), out_specs=tile_spec, check_vma=False)
```

```python
import functools

import jax
import jax.numpy as jnp
from jax import lax
from jax.experimental import pallas as pl
from jax.experimental.pallas import tpu as pltpu
from jax.sharding import PartitionSpec as P


LN_EPS = 1e-5
MASKED = -1e9
SAFE = 1e-15
MESH = pl.DeviceIdType.MESH
GROUP = 32
QTILE = 768
KEYBLK = 256
EARLY = 4
VMEM_ALL = 67043328
PAIR = 4
UNROLL = 4
SHARES = (2, 1)


def exchange_kernel(n_col, n_row, z_hbm, gamma_ref, beta_ref, wrep_ref,
                    rows_ref, ball_ref, zv, av, bt, wexp_ref, load_sem, asend, arecv, bsend, brecv, own_sem):
    me = lax.axis_index('col')
    row = lax.axis_index('row')
    parts, rows, width, chan = zv.shape
    n_chip = n_col // 2
    partner = me + 1 - 2 * lax.rem(me, 2)

    loads = []
    order = [2, n_col - 2, 1, n_col - 1]
    order += [k for k in range(1, n_col) if k not in order] + [0]
    dests = [lax.rem(me + k, n_col) for k in order]
    for slot, dest in enumerate(dests):
        load = pltpu.make_async_copy(z_hbm.at[dest], zv.at[slot], load_sem.at[slot])
        load.start()
        loads.append(load)

    barrier = pltpu.get_barrier_semaphore()
    for k in range(1, n_col):
        pl.semaphore_signal(barrier, inc=1, device_id={'col': lax.rem(me + k, n_col)}, device_id_type=MESH)
    for k in range(1, n_row):
        pl.semaphore_signal(barrier, inc=1, device_id={'row': lax.rem(row + k, n_row)}, device_id_type=MESH)
    pl.semaphore_wait(barrier, n_col + n_row - 2)

    stat = jnp.full((2 * chan, chan), 1.0 / chan, jnp.bfloat16)
    gamma = gamma_ref[...]
    beta = beta_ref[...]
    step_rows = rows

    def norm_part(slot, dest):
        def body(step, carry):
            base = step * step_rows
            z_bf = zv[slot, pl.ds(base, step_rows)].reshape(step_rows * width, chan)
            mean = jnp.dot(z_bf, stat[:chan], preferred_element_type=jnp.float32)
            cent = z_bf.astype(jnp.float32) - mean
            sq = cent * cent
            hi = sq.astype(jnp.bfloat16)
            lo = (sq - hi.astype(jnp.float32)).astype(jnp.bfloat16)
            var = jnp.dot(jnp.concatenate([hi, lo], axis=-1), stat, preferred_element_type=jnp.float32)
            normed = cent * lax.rsqrt(var + LN_EPS) * gamma + beta
            av[dest, pl.ds(base, step_rows)] = normed.astype(jnp.bfloat16).reshape(step_rows, width, chan)
            return carry

        lax.fori_loop(0, rows // step_rows, body, 0)

    def row_copy(slot):
        dest = dests[slot]
        return pltpu.make_async_remote_copy(
            av.at[dest], rows_ref.at[me], asend.at[slot], arecv.at[slot],
            device_id={'col': dest}, device_id_type=MESH)

    early = EARLY
    for slot, dest in enumerate(dests):
        loads[slot].wait()
        norm_part(slot, dest)
        if slot < early:
            row_copy(slot).start()
    own = pltpu.make_async_copy(av.at[me], rows_ref.at[me], own_sem.at[0])
    own.start()

    lane = lax.broadcasted_iota(jnp.int32, wrep_ref.shape, 1)
    for jj in range(GROUP):
        wexp_ref[jj * chan:(jj + 1) * chan] = jnp.where(lax.rem(lane, GROUP) == jj, wrep_ref[...], 0.0).astype(jnp.bfloat16)
    tile_rows = parts * rows
    heads = bt.shape[0]
    for grp in range(tile_rows // GROUP):
        flat = [av[(grp * GROUP + jj) // rows, (grp * GROUP + jj) % rows] for jj in range(GROUP)]
        res = jnp.dot(jnp.concatenate(flat, axis=-1), wexp_ref[...], preferred_element_type=jnp.float32)
        for h in range(heads):
            bt[h, :, grp * GROUP:(grp + 1) * GROUP] = res[:, h * GROUP:(h + 1) * GROUP].astype(jnp.bfloat16)

    own_b = pltpu.make_async_copy(bt, ball_ref.at[row, me], own_sem.at[1])
    own_b.start()

    def b_copy(src, src_row, src_col, kind, device):
        return pltpu.make_async_remote_copy(
            src, ball_ref.at[src_row, src_col], bsend.at[kind], brecv.at[kind],
            device_id=device, device_id_type=MESH)

    x_slot = lambda m: m - 1
    y_slot = lambda s, m: (n_chip - 1) + (s - 1) * n_chip + m
    p_slot = lambda s, m: (n_chip - 1) + (n_row - 1) * n_chip + s * n_chip + m
    sent = []
    for m in range(1, n_chip):
        cp = b_copy(bt, row, me, x_slot(m), {'col': lax.rem(me + 2 * m, n_col)})
        cp.start()
        sent.append(cp)
    for s in range(1, n_row):
        cp = b_copy(bt, row, me, y_slot(s, 0), {'row': lax.rem(row + s, n_row)})
        cp.start()
        sent.append(cp)
    cp = b_copy(bt, row, me, p_slot(0, 0), {'col': partner})
    cp.start()
    sent.append(cp)
    for slot in range(early, n_col - 1):
        row_copy(slot).start()

    def block_at(s, m):
        src_row = lax.rem(row + n_row - s, n_row)
        src_col = lax.rem(me + n_col - 2 * m, n_col)
        return src_row, src_col

    for m in range(1, n_chip):
        src_row, src_col = block_at(0, m)
        block = ball_ref.at[src_row, src_col]
        pltpu.make_async_remote_copy(block, block, bsend.at[x_slot(m)], brecv.at[x_slot(m)],
                                     device_id={'col': partner}, device_id_type=MESH).wait_recv()
        for s in range(1, n_row):
            cp = b_copy(block, src_row, src_col, y_slot(s, m), {'row': lax.rem(row + s, n_row)})
            cp.start()
            sent.append(cp)
        cp = b_copy(block, src_row, src_col, p_slot(0, m), {'col': partner})
        cp.start()
        sent.append(cp)
    for m in range(n_chip):
        for s in range(1, n_row):
            src_row, src_col = block_at(s, m)
            block = ball_ref.at[src_row, src_col]
            pltpu.make_async_remote_copy(block, block, bsend.at[y_slot(s, m)], brecv.at[y_slot(s, m)],
                                         device_id={'col': partner}, device_id_type=MESH).wait_recv()
            cp = b_copy(block, src_row, src_col, p_slot(s, m), {'col': partner})
            cp.start()
            sent.append(cp)
    for m in range(n_chip):
        for s in range(n_row):
            src_row = lax.rem(row + n_row - s, n_row)
            src_col = lax.rem(partner + n_col - 2 * m, n_col)
            block = ball_ref.at[src_row, src_col]
            pltpu.make_async_remote_copy(block, block, bsend.at[p_slot(s, m)], brecv.at[p_slot(s, m)],
                                         device_id={'col': partner}, device_id_type=MESH).wait_recv()
    for cp in sent:
        cp.wait_send()
    own_b.wait()
    own.wait()
    for slot in range(n_col - 1):
        row_copy(slot).wait()


def exchange(n_col, n_row, pair_tile, gamma, beta, w_rep, heads):
    row_len, width, chan = pair_tile.shape
    rows = row_len // n_col
    n_bsem = (n_col // 2 - 1) + (n_row - 1) * (n_col // 2) + n_row * (n_col // 2)
    hbm = pl.BlockSpec(memory_space=pl.ANY)
    vmem = pl.BlockSpec(memory_space=pltpu.VMEM)
    return pl.pallas_call(
        functools.partial(exchange_kernel, n_col, n_row),
        name='exchange_rows',
        out_shape=(jax.ShapeDtypeStruct((n_col, rows, width, chan), jnp.bfloat16),
                   jax.ShapeDtypeStruct((n_row, n_col, heads, width, row_len), jnp.bfloat16)),
        in_specs=[hbm, vmem, vmem, vmem],
        out_specs=(hbm, hbm),
        scratch_shapes=[
            pltpu.VMEM((n_col, rows, width, chan), jnp.bfloat16),
            pltpu.VMEM((n_col, rows, width, chan), jnp.bfloat16),
            pltpu.VMEM((heads, width, row_len), jnp.bfloat16),
            pltpu.VMEM((GROUP * chan, heads * GROUP), jnp.bfloat16),
            pltpu.SemaphoreType.DMA((n_col,)),
            pltpu.SemaphoreType.DMA((n_col,)),
            pltpu.SemaphoreType.DMA((n_col,)),
            pltpu.SemaphoreType.DMA((n_bsem,)),
            pltpu.SemaphoreType.DMA((n_bsem,)),
            pltpu.SemaphoreType.DMA((2,)),
        ],
        compiler_params=pltpu.CompilerParams(collective_id=1, has_side_effects=True, vmem_limit_bytes=VMEM_ALL),
    )(pair_tile.reshape(n_col, rows, width, chan), gamma, beta, w_rep)


def attend_kernel(scale, a_ref, ball_ref, mask_ref, wq_ref, wk_ref, wv_ref, wg_ref, out_ref,
                  wqvg_ref, bias, kbuf, qz, vt, gt, og, edge, mcol):
    n_row, n_col, heads, width, row_len = ball_ref.shape
    keys = n_col * width
    chan = a_ref.shape[-1]
    head_dim = chan // heads

    @pl.when(pl.program_id(0) == 0)
    def _():
        qz[...] = jnp.zeros_like(qz)
        for n, w_ref in enumerate((wq_ref, wv_ref, wg_ref)):
            wqvg_ref[n * chan:(n + 1) * chan] = w_ref[...].astype(jnp.float32).T.astype(jnp.bfloat16)
        added = jnp.where(mask_ref[...] > 0, 0.0, MASKED).astype(jnp.float32)
        mcol[...] = jnp.broadcast_to(added, (chan, keys)).T

        def fill(c, carry):
            krange = pl.ds(pl.multiple_of(c * width, width), width)
            mask = mcol[krange, :1]
            for h in range(heads):
                for r in range(n_row):
                    bias[h, krange, r * row_len:(r + 1) * row_len] = ball_ref[r, c, h].astype(jnp.float32) + mask
            return carry

        lax.fori_loop(0, n_col, fill, 0)

    pair = a_ref.shape[1]
    for r in range(pair):
        a = a_ref[:, r].reshape(keys, chan)
        kbuf[r] = jnp.dot(a, wk_ref[...], preferred_element_type=jnp.float32).astype(jnp.bfloat16)
        qvg = lax.dot_general(wqvg_ref[...], a, (((1,), (1,)), ((), ())), preferred_element_type=jnp.float32)
        q_t = (qvg[:chan] * scale).astype(jnp.bfloat16)
        v_t = qvg[chan:2 * chan].astype(jnp.bfloat16)
        gt[r] = jax.nn.sigmoid(qvg[2 * chan:]).reshape(heads, head_dim, keys)
        for h in range(heads):
            qz[r, h, h * head_dim:(h + 1) * head_dim, :] = q_t[h * head_dim:(h + 1) * head_dim]
            vt[r, h] = v_t[h * head_dim:(h + 1) * head_dim]

    def attend(nk):
        def heads_of(step, worst):
            low, high = worst
            r = step // (heads // UNROLL)
            for u in range(UNROLL):
                h = lax.rem(step, heads // UNROLL) * UNROLL + u
                for qt in range(keys // QTILE):
                    cols = slice(qt * QTILE, (qt + 1) * QTILE)
                    q_h = qz[r, h, :, cols]
                    total = None
                    parts = []
                    for kb in range(nk // KEYBLK):
                        kr = slice(kb * KEYBLK, (kb + 1) * KEYBLK)
                        s = jnp.dot(kbuf[r, kr], q_h, preferred_element_type=jnp.float32) + bias[h, kr, cols]
                        p = jnp.exp(s)
                        fold = jnp.sum(p.reshape(KEYBLK // 8, 8, QTILE), axis=0)
                        total = fold if total is None else total + fold
                        parts.append(p.astype(jnp.bfloat16))
                    l = jnp.sum(total, axis=0, keepdims=True)
                    o = jnp.dot(vt[r, h, :, :nk], jnp.concatenate(parts, axis=0), preferred_element_type=jnp.float32)
                    og[r, h, :, cols] = gt[r, h, :, cols] * (o / l)
                    low = jnp.minimum(low, l)
                    high = jnp.maximum(high, jnp.maximum(l, jnp.max(jnp.abs(o), axis=0, keepdims=True)))
            return low, high

        low, high = lax.fori_loop(0, pair * heads // UNROLL, heads_of, (jnp.full((1, QTILE), 1.0, jnp.float32),) * 2)
        edge[0:1] = low
        edge[1:2] = 1.0 / high

    def attend_exact(nk):
        def head(step, carry):
            r, h = step // heads, lax.rem(step, heads)
            for qt in range(keys // QTILE):
                cols = slice(qt * QTILE, (qt + 1) * QTILE)
                s = jnp.dot(kbuf[r, :nk], qz[r, h, :, cols], preferred_element_type=jnp.float32) + bias[h, :nk, cols]
                m = jnp.max(s, axis=0, keepdims=True)
                p = jnp.exp(s - m)
                l = jnp.sum(p, axis=0, keepdims=True)
                o = jnp.dot(vt[r, h, :, :nk], p.astype(jnp.bfloat16), preferred_element_type=jnp.float32)
                og[r, h, :, cols] = gt[r, h, :, cols] * (o / l)
            return carry

        lax.fori_loop(0, pair * heads, head, 0)

    attend(keys)

    @pl.when(jnp.logical_not(jnp.min(edge[...]) > SAFE))
    def _():
        attend_exact(keys)

    for r in range(pair):
        gated = og[r].reshape(chan, keys).T
        out_ref[:, r] = gated.astype(jnp.bfloat16).reshape(n_col, width, chan)


def attend(first, count, a_rows, ball, mask, weights, scale):
    n_col, _, width, chan = a_rows.shape
    _, _, heads, _, _ = ball.shape
    keys = n_col * width
    head_dim = chan // heads
    const = lambda shape: pl.BlockSpec(shape, lambda g: (0,) * len(shape), pipeline_mode=pl.Buffered(1))
    grid_spec = pltpu.PrefetchScalarGridSpec(
        num_scalar_prefetch=0,
        grid=(count // PAIR,),
        in_specs=[
            pl.BlockSpec((n_col, PAIR, width, chan), lambda g: (0, first // PAIR + g, 0, 0)),
            const(ball.shape), const(mask.shape), *[const(w.shape) for w in weights],
        ],
        out_specs=pl.BlockSpec((n_col, PAIR, width, chan), lambda g: (0, g, 0, 0)),
        scratch_shapes=[
            pltpu.VMEM((3 * chan, chan), jnp.bfloat16),
            pltpu.VMEM((heads, keys, keys), jnp.float32),
            pltpu.VMEM((PAIR, keys, chan), jnp.bfloat16),
            pltpu.VMEM((PAIR, heads, chan, keys), jnp.bfloat16),
            pltpu.VMEM((PAIR, heads, head_dim, keys), jnp.bfloat16),
            pltpu.VMEM((PAIR, heads, head_dim, keys), jnp.float32),
            pltpu.VMEM((PAIR, heads, head_dim, keys), jnp.float32),
            pltpu.VMEM((2, QTILE), jnp.float32),
            pltpu.VMEM((keys, chan), jnp.float32),
        ])
    flops = count * (4 * keys * keys * chan * 2 + 8 * keys * chan * chan)
    return pl.pallas_call(
        functools.partial(attend_kernel, scale),
        name='attend_rows',
        grid_spec=grid_spec,
        out_shape=jax.ShapeDtypeStruct((n_col, count, width, chan), jnp.bfloat16),
        cost_estimate=pl.CostEstimate(flops=flops * 20, bytes_accessed=ball.size * 2 + count * keys * chan * 4,
                                      transcendentals=count * heads * keys * keys),
        compiler_params=pltpu.CompilerParams(dimension_semantics=('arbitrary',), vmem_limit_bytes=VMEM_ALL),
    )(a_rows, ball, mask, *weights)


def finish_kernel(z_ref, g_ref, wo_ref, *rest):
    out_ref = rest[-1]
    parts, count, width, chan = z_ref.shape
    for d in range(parts):
        upd = jnp.dot(g_ref[d].reshape(count * width, chan), wo_ref[...], preferred_element_type=jnp.float32)
        z = z_ref[d].reshape(count * width, chan).astype(jnp.float32)
        out_ref[d] = (z + upd).astype(jnp.bfloat16).reshape(count, width, chan)


def finish(first, count, z_parts, gated, w_o, prev):
    n_col, _, width, chan = z_parts.shape
    parts = n_col // 2
    unit = 4
    blk = pl.BlockSpec((parts, unit, width, chan), lambda d, r: (d, first // unit + r, 0, 0))
    in_specs = [blk, pl.BlockSpec((parts, unit, width, chan), lambda d, r: (d, r, 0, 0)),
                pl.BlockSpec(w_o.shape, lambda d, r: (0, 0))]
    args = [z_parts, gated, w_o]
    alias = {}
    if prev is not None:
        in_specs.append(pl.BlockSpec(memory_space=pl.ANY))
        args.append(prev)
        alias = {3: 0}
    return pl.pallas_call(
        finish_kernel, name='finish_rows', grid=(n_col // parts, count // unit), in_specs=in_specs, out_specs=blk,
        out_shape=jax.ShapeDtypeStruct(z_parts.shape, z_parts.dtype),
        input_output_aliases=alias,
        cost_estimate=pl.CostEstimate(flops=n_col * count * width * chan * chan * 2 * 4, transcendentals=0,
                                      bytes_accessed=n_col * count * width * chan * 6),
        compiler_params=pltpu.CompilerParams(dimension_semantics=('arbitrary', 'arbitrary'), vmem_limit_bytes=VMEM_ALL),
    )(*args)


def solution(mesh):
    n_col, n_row = mesh.shape['col'], mesh.shape['row']
    tile_spec = P(('dp', 'row'), 'col', None)

    def per_device(pair_tile, res_mask, ln_gamma, ln_beta, w_q, w_k, w_v, w_b, w_g, w_o):
        row_len, width, chan = pair_tile.shape
        heads = w_b.shape[1]
        keys = n_col * width
        scale = (w_q.shape[1] // heads) ** -0.5
        rows = row_len // n_col
        w_rep = jnp.repeat(w_b.astype(jnp.float32), GROUP, axis=1)
        a_rows, ball = exchange(n_col, n_row, pair_tile, ln_gamma.reshape(1, chan), ln_beta.reshape(1, chan), w_rep, heads)
        mask = res_mask.reshape(1, keys)
        z_parts = pair_tile.reshape(n_col, rows, width, chan)
        home, first = [], 0
        for share in SHARES:
            count = rows * share // sum(SHARES)
            gated = attend(first, count, a_rows, ball, mask, (w_q, w_k, w_v, w_g), scale)
            home.append((first, count, lax.all_to_all(gated, 'col', 0, 0, tiled=True)))
            first += count
        out = None
        for first, count, gated in home:
            out = finish(first, count, z_parts, gated, w_o, out)
        return out.reshape(row_len, width, chan)

    return jax.shard_map(per_device, mesh=mesh, in_specs=(tile_spec, P('dp'), P(), P(), P(), P(), P(), P(), P(), P()), out_specs=tile_spec, check_vma=False)
```
